32 devices in a mesh: seq: 16 (over z, y, core), batch: 2 (over x).
Axes of the slice: x: 2, y: 2, z: 4, core: 2. Of those that a mesh axis runs over, the one named last changes fastest.
Arguments:
- hidden_in: bfloat16 [2, 4096, 2304], P('batch', 'seq'), may hold values from -6 to 6
- segment_ids: int32 [2, 4096], P('batch', 'seq'), may hold values from 0 to 15, never falling along the last dimension, each value on 1 to 512 neighbouring positions
- pre_gain: float32 [2304], replicated, may hold values from 0.25 to 1.75
- w_qkv: bfloat16 [2304, 2048], P('seq'), may hold values from -0.27083333 to 0.27083333
- w_out: bfloat16 [1024, 2304], P('seq'), may hold values from -0.1875 to 0.1875
- post_gain: float32 [2304], replicated, may hold values from 0.25 to 1.75
Outputs:
- layer_out: bfloat16 [2, 4096, 2304], P('batch', 'seq')
The draws below stay inside these ranges and needn't reach their ends.
Inputs may be any that keep to these rules, and one draw needn't show every extreme that they name: `segment_ids`: along each sequence the numbers never fall; a document is 1 to 512 positions long, and each sequence has one of exactly 512.
All inputs are finite; a program needn't handle non-finite values.
Results may differ from the reference program's by a relative error of at most 0.012.
The reference program's roundings to bfloat16 on the way (of `normed` and `attended`) count: a program that leaves them out, or rounds other values in their place, can miss the bound.
Values may be sent and summed in bfloat16 or wider, within the bound.
A program may use at most 128 MiB of HBM per device.

```python
import math
import jax
import jax.numpy as jnp
import numpy as np
from jax import lax

D = 2304
Q_HEADS = 4
KV_HEADS = 2
HEAD = 256
WINDOW = 4096
DOCS = 16
TOK_DEV = 256
SEQ = 4096
BATCH = 2
QKV_W = 2048
ATT_W = 1024
DOC_MOST = 512


def draw_w_qkv(key, part):
    base_key = jax.random.fold_in(key, 11)
    pick_key = jax.random.fold_in(key, 12)
    base = jnp.clip(jax.random.normal(base_key, (D, QKV_W), jnp.float32), -3.0, 3.0)
    order = jax.random.permutation(pick_key, KV_HEADS)
    boosted = order < (KV_HEADS + 1) // 2
    columns = jnp.arange(QKV_W, dtype=jnp.int32)
    head_of = columns // HEAD
    group_of = jnp.where(head_of < Q_HEADS, head_of // (Q_HEADS // KV_HEADS), head_of - Q_HEADS)
    group_of = jnp.clip(group_of, 0, KV_HEADS - 1)
    is_value = head_of >= Q_HEADS + KV_HEADS
    factor = jnp.where(boosted[group_of] & jnp.logical_not(is_value), 4.0, 1.0).astype(jnp.float32)
    return (base * factor[None, :] * float(D) ** (-0.5)).astype(jnp.bfloat16)


def block_levels(stream_key, dims, cuts, least, high):
    def one(position, shards_of):
        steps = jax.random.uniform(jax.random.fold_in(jax.random.fold_in(stream_key, 6), position), (shards_of,), jnp.float32, least / len(cuts), high / len(cuts))
        return jnp.repeat(jnp.exp(steps), dims[position] // shards_of).reshape((-1,) + (1,) * (len(dims) - position - 1))

    factor_of = one(*cuts[0])
    for cut in cuts[1:]:
        factor_of = factor_of * one(*cut)
    return factor_of


def profile(count, total, limit, lean):
    weights = [(1 << 20) // math.isqrt(standing ** lean) + 1 for standing in range(2, count + 1)]
    rest, given = total - limit - (count - 1), [1] * (count - 1)
    while rest > 0:
        free = [i for i in range(count - 1) if given[i] < limit]
        whole, budget = sum([weights[i] for i in free]), rest
        for i in free:
            addition = min(limit - given[i], max(1, budget * weights[i] // whole), rest)
            given[i] = given[i] + addition
            rest = rest - addition
    return np.array([limit] + given)


def uneven(own_key, count, total, bound, skew):
    if count == 2:
        one = jax.random.randint(own_key, (), max(1, total - bound), min(bound, total - 1) + 1)
        return jnp.stack([one, total - one])
    sizes = jnp.asarray(profile(count, total, bound, skew), jnp.int32)
    pairs = (count - 1) // 2
    source_of, taker = sizes[1:1 + 2 * pairs:2], sizes[2:2 + 2 * pairs:2]
    margin = jnp.minimum(source_of - 1, bound - taker)
    passed = jax.random.randint(jax.random.fold_in(own_key, 1), (pairs,), 0, 1 << 20) % (margin + 1)
    sizes = sizes.at[1:1 + 2 * pairs:2].set(source_of - passed).at[2:2 + 2 * pairs:2].set(taker + passed)
    return sizes[jax.random.permutation(jax.random.fold_in(own_key, 2), count)]


def normal_values(own_key, dims, width, most, cuts=(), held_as=jnp.bfloat16):
    values = jax.random.normal(own_key, dims, jnp.float32) * width
    if len(cuts) > 0:
        values = block_levels(own_key, dims, cuts, -0.22, 0.18) * values
    return jnp.clip(values, min=-most, max=most).astype(held_as)


def setup_inputs(seed: int = 0) -> dict:
    arg_keys = jax.random.split(jax.random.key(seed), 7)
    hidden_in = normal_values(arg_keys[0], (BATCH, SEQ, D), 1.0, 6.0, ((0, 2), (1, 16)))
    segment_ids = jax.vmap(lambda own: jnp.searchsorted(jnp.cumsum(uneven(own, DOCS, SEQ, DOC_MOST, 2)), jnp.arange(SEQ), side="right"))(jax.random.split(arg_keys[1], BATCH)).reshape((BATCH, SEQ)).astype(jnp.int32)
    pre_gain = jnp.clip(1.0 + 0.15 * jax.random.normal(arg_keys[2], (D,), jnp.float32), 0.25, 1.75)
    w_qkv = draw_w_qkv(jax.random.fold_in(arg_keys[6], 71), 0)
    w_out = normal_values(arg_keys[4], (ATT_W, D), ATT_W ** -0.5, 0.1875, ((0, 16),))
    post_gain = jnp.clip(1.0 + 0.15 * jax.random.normal(arg_keys[5], (D,), jnp.float32), 0.25, 1.75)
    return dict(hidden_in=hidden_in, segment_ids=segment_ids, pre_gain=pre_gain, w_qkv=w_qkv, w_out=w_out, post_gain=post_gain)


EPS = 1e-06
CAP = 50.0

def rms_scale(values, gain):
    return values * lax.rsqrt(lax.optimization_barrier(jnp.mean(values * values, axis=-1, keepdims=True)) + EPS) * gain

def barrier_round(values):
    return lax.optimization_barrier(values.astype(jnp.bfloat16)).astype(jnp.float32)

def rotary(values, positions):
    head_size = values.shape[-1]
    half_dim = head_size // 2
    inverse = 1.0 / 10000.0 ** (jnp.arange(half_dim, dtype=jnp.float32) * 2.0 / head_size)
    angles = positions.astype(jnp.float32)[:, None] * inverse[None, :]
    shape = (values.shape[0],) + (1,) * (values.ndim - 2) + (half_dim,)
    cosine = jnp.cos(angles).reshape(shape)
    sine = jnp.sin(angles).reshape(shape)
    first_half = values[..., :half_dim]
    second_half = values[..., half_dim:]
    return jnp.concatenate([first_half * cosine - second_half * sine, second_half * cosine + first_half * sine], axis=-1)

def one_sequence(inputs, segment_row, pre_gain, w_qkv, w_out, post_gain):
    seq_len = inputs.shape[0]
    groups = Q_HEADS // KV_HEADS
    widened = inputs.astype(jnp.float32)
    normed = rms_scale(widened, pre_gain).astype(jnp.bfloat16)
    projected = jnp.dot(normed, w_qkv, preferred_element_type=jnp.float32)
    positions = jnp.arange(seq_len, dtype=jnp.int32)
    queries = rotary(projected[:, :Q_HEADS * HEAD].reshape(seq_len, KV_HEADS, groups, HEAD), positions)
    key_rows = rotary(projected[:, Q_HEADS * HEAD:(Q_HEADS + KV_HEADS) * HEAD].reshape(seq_len, KV_HEADS, HEAD), positions)
    value_rows = projected[:, (Q_HEADS + KV_HEADS) * HEAD:].reshape(seq_len, KV_HEADS, HEAD)
    query_full = barrier_round(queries)
    key_full = barrier_round(key_rows)
    value_full = barrier_round(value_rows)
    doc_numbers = jnp.arange(DOCS, dtype=jnp.int32)
    matches = segment_row[:, None] == doc_numbers[None, :]
    first_pos = lax.optimization_barrier(jnp.min(jnp.where(matches, positions[:, None], seq_len), axis=0)).astype(jnp.int32)
    starts = lax.optimization_barrier(jnp.sum(jnp.where(matches, first_pos[None, :], 0), axis=1)).astype(jnp.int32)
    key_pad = jnp.concatenate([jnp.zeros((WINDOW, KV_HEADS, HEAD), jnp.float32), key_full], axis=0)
    value_pad = jnp.concatenate([jnp.zeros((WINDOW, KV_HEADS, HEAD), jnp.float32), value_full], axis=0)
    scale = 1.0 / math.sqrt(HEAD)

    def block(index):
        qstart = (index * TOK_DEV).astype(jnp.int32)
        query_block = lax.dynamic_slice_in_dim(query_full, qstart, TOK_DEV, 0)
        key_block = lax.dynamic_slice_in_dim(key_pad, qstart, WINDOW + TOK_DEV, 0)
        value_block = lax.dynamic_slice_in_dim(value_pad, qstart, WINDOW + TOK_DEV, 0)
        start_block = lax.dynamic_slice_in_dim(starts, qstart, TOK_DEV, 0)
        query_pos = qstart + jnp.arange(TOK_DEV, dtype=jnp.int32)
        key_pos = qstart - WINDOW + jnp.arange(WINDOW + TOK_DEV, dtype=jnp.int32)
        scores = jnp.einsum('qhgd,khd->qhgk', query_block, key_block) * scale
        capped = CAP * jnp.tanh(scores / CAP)
        allowed = (key_pos[None, :] <= query_pos[:, None]) & (query_pos[:, None] - key_pos[None, :] < WINDOW) & (key_pos[None, :] >= start_block[:, None])
        weights = jnp.where(allowed[:, None, None, :], jnp.exp(capped), 0.0)
        totals = lax.optimization_barrier(jnp.sum(weights, axis=-1))
        mixed = jnp.einsum('qhgk,khd->qhgd', barrier_round(weights), value_block)
        return (mixed / totals[..., None]).astype(jnp.bfloat16).reshape(TOK_DEV, Q_HEADS * HEAD)
    attended = lax.map(block, jnp.arange(seq_len // TOK_DEV, dtype=jnp.int32)).reshape(seq_len, Q_HEADS * HEAD)
    branch = jnp.dot(attended, w_out, preferred_element_type=jnp.float32)
    return (widened + rms_scale(branch, post_gain)).astype(jnp.bfloat16)

def reference(hidden_in, segment_ids, pre_gain, w_qkv, w_out, post_gain):
    results = []
    for row in range(BATCH):
        results.append(one_sequence(hidden_in[row], segment_ids[row], pre_gain, w_qkv, w_out, post_gain))
    return jnp.stack(results, axis=0)
```

```python
import math

import jax
import jax.numpy as jnp
from jax import lax
from jax.sharding import PartitionSpec as P

Q_HEADS = 4
KV_HEADS = 2
HEAD = 256
WINDOW = 4096
DOCS = 16


EPS = 1e-06
CAP = 50.0


def from_behind(block, axis, distance):
    devices = range(lax.axis_size(axis))
    route = [(i - distance, i) for i in devices if i - distance in devices]
    return lax.ppermute(block, axis, route)


def rms_scale(values, gain):
    return values * lax.rsqrt(jnp.mean(values * values, axis=-1, keepdims=True) + EPS) * gain


def rotary(values, positions, leading):
    head_size = values.shape[-1]
    half_dim = head_size // 2
    inverse = 1.0 / 10000.0 ** (jnp.arange(half_dim, dtype=jnp.float32) * 2.0 / head_size)
    angles = positions.astype(jnp.float32)[:, None] * inverse[None, :]
    shape = (
        (1,) * leading + (positions.shape[0],) + (1,) * (values.ndim - 2 - leading) + (half_dim,)
    )
    cosine = jnp.cos(angles).reshape(shape)
    sine = jnp.sin(angles).reshape(shape)
    first_half = values[..., :half_dim]
    second_half = values[..., half_dim:]
    return jnp.concatenate(
        [first_half * cosine - second_half * sine, second_half * cosine + first_half * sine],
        axis=-1,
    )


def per_device(hidden_in, segment_ids, pre_gain, w_qkv, w_out, post_gain):
    tok_rows = hidden_in.shape[1]
    seq_count = lax.axis_size("seq")
    seq_index = lax.axis_index("seq")
    groups = Q_HEADS // KV_HEADS
    doc_most = min(WINDOW, seq_count * tok_rows // 8)
    hops = min(-(-(doc_most - 1) // tok_rows), seq_count - 1)
    positions = seq_index * tok_rows + jnp.arange(tok_rows, dtype=jnp.int32)
    own_ids = segment_ids[0]
    id_blocks = [from_behind(own_ids, "seq", d) for d in range(hops, 0, -1)] + [own_ids]
    widened = hidden_in[0].astype(jnp.float32)
    normed = rms_scale(widened, pre_gain).astype(jnp.bfloat16)
    projected = jnp.dot(
        normed,
        lax.all_gather(w_qkv, "seq", axis=0, tiled=True),
        preferred_element_type=jnp.float32,
    )
    queries = rotary(
        projected[:, : Q_HEADS * HEAD].reshape(tok_rows, KV_HEADS, groups, HEAD), positions, 0
    ).astype(jnp.bfloat16)
    key_rows = rotary(
        projected[:, Q_HEADS * HEAD : (Q_HEADS + KV_HEADS) * HEAD].reshape(
            tok_rows, KV_HEADS, HEAD
        ),
        positions,
        0,
    ).astype(jnp.bfloat16)
    value_rows = projected[:, (Q_HEADS + KV_HEADS) * HEAD :].astype(jnp.bfloat16)
    both = jnp.concatenate([key_rows.reshape(tok_rows, KV_HEADS * HEAD), value_rows], axis=1)
    blocks = [from_behind(both, "seq", d) for d in range(hops, 0, -1)] + [both]
    kv = jnp.concatenate(blocks, axis=0).reshape(-1, 2, KV_HEADS, HEAD)
    ids = jnp.concatenate(id_blocks, axis=0)
    key_pos = (seq_index - hops) * tok_rows + jnp.arange((hops + 1) * tok_rows, dtype=jnp.int32)
    allowed = (
        (key_pos[None, :] >= 0)
        & (key_pos[None, :] <= positions[:, None])
        & (positions[:, None] - key_pos[None, :] < WINDOW)
        & (ids[None, :] == own_ids[:, None])
    )
    scores = jnp.einsum(
        "qhgd,khd->hgqk", queries, kv[:, 0], preferred_element_type=jnp.float32
    ) * (1.0 / math.sqrt(HEAD))
    capped = CAP * jnp.tanh(scores / CAP)
    weights = jnp.where(allowed[None, None], jnp.exp(capped), 0.0)
    totals = jnp.sum(weights, axis=-1)
    mixed = jnp.einsum(
        "hgqk,khd->hgqd", weights.astype(jnp.bfloat16), kv[:, 1], preferred_element_type=jnp.float32
    )
    attended = (mixed / totals[..., None]).astype(jnp.bfloat16)
    attended = attended.transpose(2, 0, 1, 3).reshape(tok_rows, Q_HEADS * HEAD)
    branch = jnp.dot(
        attended,
        lax.all_gather(w_out, "seq", axis=0, tiled=True),
        preferred_element_type=jnp.float32,
    )
    return (widened + rms_scale(branch, post_gain)).astype(jnp.bfloat16)[None]


def solution(mesh):
    placed = (P("batch", "seq", None), P("batch", "seq"), P(), P("seq", None), P("seq", None), P())
    return jax.shard_map(
        per_device, mesh=mesh, in_specs=placed, out_specs=P("batch", "seq", None), check_vma=False
    )
```

```python
import functools
import math

import jax
import jax.numpy as jnp
from jax import lax
from jax.experimental import pallas as pl
from jax.experimental.pallas import tpu as pltpu
from jax.sharding import PartitionSpec as P

Q_HEADS = 4
KV_HEADS = 2
HEAD = 256
WINDOW = 4096
DOCS = 16


EPS = 1e-06
CAP = 50.0


def from_behind(block, axis, distance):
    devices = range(lax.axis_size(axis))
    route = [(i - distance, i) for i in devices if i - distance in devices]
    return lax.ppermute(block, axis, route)


def rms_scale(values, gain):
    return values * lax.rsqrt(jnp.mean(values * values, axis=-1, keepdims=True) + EPS) * gain


def rotary(values, positions, leading):
    head_size = values.shape[-1]
    half_dim = head_size // 2
    inverse = 1.0 / 10000.0 ** (jnp.arange(half_dim, dtype=jnp.float32) * 2.0 / head_size)
    angles = positions.astype(jnp.float32)[:, None] * inverse[None, :]
    shape = (
        (1,) * leading + (positions.shape[0],) + (1,) * (values.ndim - 2 - leading) + (half_dim,)
    )
    cosine = jnp.cos(angles).reshape(shape)
    sine = jnp.sin(angles).reshape(shape)
    first_half = values[..., :half_dim]
    second_half = values[..., half_dim:]
    return jnp.concatenate(
        [first_half * cosine - second_half * sine, second_half * cosine + first_half * sine],
        axis=-1,
    )


def plain_layer(hidden_in, segment_ids, pre_gain, w_qkv, w_out, post_gain):
    tok_rows = hidden_in.shape[1]
    seq_count = lax.axis_size("seq")
    seq_index = lax.axis_index("seq")
    groups = Q_HEADS // KV_HEADS
    doc_most = min(WINDOW, seq_count * tok_rows // 8)
    hops = min(-(-(doc_most - 1) // tok_rows), seq_count - 1)
    positions = seq_index * tok_rows + jnp.arange(tok_rows, dtype=jnp.int32)
    own_ids = segment_ids[0]
    id_blocks = [from_behind(own_ids, "seq", d) for d in range(hops, 0, -1)] + [own_ids]
    widened = hidden_in[0].astype(jnp.float32)
    normed = rms_scale(widened, pre_gain).astype(jnp.bfloat16)
    projected = jnp.dot(
        normed,
        lax.all_gather(w_qkv, "seq", axis=0, tiled=True),
        preferred_element_type=jnp.float32,
    )
    queries = rotary(
        projected[:, : Q_HEADS * HEAD].reshape(tok_rows, KV_HEADS, groups, HEAD), positions, 0
    ).astype(jnp.bfloat16)
    key_rows = rotary(
        projected[:, Q_HEADS * HEAD : (Q_HEADS + KV_HEADS) * HEAD].reshape(
            tok_rows, KV_HEADS, HEAD
        ),
        positions,
        0,
    ).astype(jnp.bfloat16)
    value_rows = projected[:, (Q_HEADS + KV_HEADS) * HEAD :].astype(jnp.bfloat16)
    both = jnp.concatenate([key_rows.reshape(tok_rows, KV_HEADS * HEAD), value_rows], axis=1)
    blocks = [from_behind(both, "seq", d) for d in range(hops, 0, -1)] + [both]
    kv = jnp.concatenate(blocks, axis=0).reshape(-1, 2, KV_HEADS, HEAD)
    ids = jnp.concatenate(id_blocks, axis=0)
    key_pos = (seq_index - hops) * tok_rows + jnp.arange((hops + 1) * tok_rows, dtype=jnp.int32)
    allowed = (
        (key_pos[None, :] >= 0)
        & (key_pos[None, :] <= positions[:, None])
        & (positions[:, None] - key_pos[None, :] < WINDOW)
        & (ids[None, :] == own_ids[:, None])
    )
    scores = jnp.einsum(
        "qhgd,khd->hgqk", queries, kv[:, 0], preferred_element_type=jnp.float32
    ) * (1.0 / math.sqrt(HEAD))
    capped = CAP * jnp.tanh(scores / CAP)
    weights = jnp.where(allowed[None, None], jnp.exp(capped), 0.0)
    totals = jnp.sum(weights, axis=-1)
    mixed = jnp.einsum(
        "hgqk,khd->hgqd", weights.astype(jnp.bfloat16), kv[:, 1], preferred_element_type=jnp.float32
    )
    attended = (mixed / totals[..., None]).astype(jnp.bfloat16)
    attended = attended.transpose(2, 0, 1, 3).reshape(tok_rows, Q_HEADS * HEAD)
    branch = jnp.dot(
        attended,
        lax.all_gather(w_out, "seq", axis=0, tiled=True),
        preferred_element_type=jnp.float32,
    )
    return (widened + rms_scale(branch, post_gain)).astype(jnp.bfloat16)[None]


class Gather:
    def __init__(self, place, own_ref, full_ref, piece, send_sems, recv_sems):
        self.place, self.own_ref, self.full_ref = place, own_ref, full_ref
        self.piece, self.send_sems, self.recv_sems = piece, send_sems, recv_sems
        self.steps = place["chips"] - 1
        self.started = []

    def slot(self, kind, hop, unit):
        return (kind * self.steps + hop - 1) * 2 + unit

    def spot(self, kind, hop, core, unit):
        place = self.place
        shift = -hop if kind == 0 else hop
        third = (1, 2 * place["x"], 2 - 2 * place["x"])[kind]
        device = place["chip_at"](place["ring"] + shift) * 2 + core
        return self.piece(self.full_ref, device, third, unit)

    def copy(self, source, target, slot, device):
        return pltpu.make_async_remote_copy(
            src_ref=source,
            dst_ref=target,
            send_sem=self.send_sems.at[slot],
            recv_sem=self.recv_sems.at[slot],
            device_id=device,
            device_id_type=pl.DeviceIdType.MESH,
        )

    def send(self, source, target, slot, device):
        moving = self.copy(source, target, slot, device)
        moving.start()
        self.started.append(moving)

    def arrived(self, spot, slot):
        self.copy(spot, spot, slot, self.place["sibling"]).wait_recv()

    def first_hop(self):
        place = self.place
        for unit in range(2):
            for kind, target in ((0, place["up"]), (1, place["down"])):
                third = (1, 2 * place["x"])[kind]
                self.send(
                    self.piece(self.own_ref, 0, third, unit),
                    self.piece(self.full_ref, place["seq"], third, unit),
                    self.slot(kind, 1, unit),
                    target,
                )

    def share_own(self):
        rows = self.own_ref.shape[0]
        mine = self.full_ref.at[pl.ds(pl.multiple_of(self.place["seq"] * rows, 16), rows), :]
        self.send(self.own_ref, mine, 12 * self.steps, self.place["sibling"])

    def relay(self, kind, hop, unit):
        spot = self.spot(kind, hop, self.place["core"], unit)
        self.send(spot, spot, self.slot(kind + 3, hop, unit), self.place["sibling"])

    def take_x(self, hop):
        for unit in range(2):
            self.arrived(self.spot(2, hop, self.place["core"], unit), self.slot(2, hop, unit))
            self.relay(2, hop, unit)

    def step(self, hop):
        place = self.place
        for unit in range(2):
            for kind, target in ((0, place["up"]), (1, place["down"])):
                spot = self.spot(kind, hop, place["core"], unit)
                self.arrived(spot, self.slot(kind, hop, unit))
                if hop < self.steps:
                    self.send(spot, spot, self.slot(kind, hop + 1, unit), target)
                if kind == 1:
                    self.send(spot, spot, self.slot(2, hop, unit), place["across"])
                self.relay(kind, hop, unit)
        if hop > 1:
            self.take_x(hop - 1)

    def finish(self):
        self.take_x(self.steps)
        other = 1 - self.place["core"]
        for hop in range(1, self.steps + 1):
            for kind in range(3):
                for unit in range(2):
                    self.arrived(self.spot(kind, hop, other, unit), self.slot(kind + 3, hop, unit))
        rows = self.own_ref.shape[0]
        start = (self.place["seq"] + 1 - 2 * self.place["core"]) * rows
        theirs = self.full_ref.at[pl.ds(pl.multiple_of(start, 16), rows), :]
        self.arrived(theirs, 12 * self.steps)

    def drain(self):
        for moving in self.started:
            moving.wait_send()


def make_piece(rows, width, by_rows):
    def piece(ref, device, third, unit):
        if by_rows:
            part, columns = rows // 3, width // 2
            return ref.at[
                pl.ds(pl.multiple_of(device * rows + third * part, 16), part),
                pl.ds(unit * columns, columns),
            ]
        columns = width // 6
        return ref.at[
            pl.ds(pl.multiple_of(device * rows, 16), rows),
            pl.ds(pl.multiple_of(third * 2 * columns + unit * columns, 128), columns),
        ]

    return piece


def layer_kernel(
    chips, hid, ids_row, ids_col, cos, sin, pre, w_qkv, w_out, post, out,
    wq, wo, nrm, qry, kv, kv1, kv2, id1, id2, acc, tot, att, branch,
    q_send, q_recv, o_send, o_recv, s_send, s_recv, local_sem,
):
    seq, x = lax.axis_index("seq"), lax.axis_index("batch")
    chip, core = seq // 2, seq % 2
    half = chips // 2
    layer, side = chip // 2, chip % 2
    ring = (1 - side) * layer + side * (chips - 1 - layer)

    def chip_at(position):
        position = (position + chips) % chips
        far = position // half
        return (1 - far) * 2 * position + far * (2 * (chips - 1 - position) + 1)

    def at(device_chip, device_core, batch):
        return {"seq": device_chip * 2 + device_core, "batch": batch}

    place = dict(
        chips=chips, seq=seq, x=x, core=core, ring=ring, chip_at=chip_at,
        sibling=at(chip, 1 - core, x), across=at(chip, core, 1 - x),
        up=at(chip_at(ring + 1), core, x), down=at(chip_at(ring - 1), core, x),
    )
    after = at((chip + 1) % chips, core, x)
    before = at((chip + chips - 1) % chips, core, x)
    met = [place["sibling"], place["across"], place["up"], place["down"], after, before]
    barrier = pltpu.get_barrier_semaphore()
    for other in met:
        pl.semaphore_signal(barrier, 1, device_id=other, device_id_type=pl.DeviceIdType.MESH)
    pl.semaphore_wait(barrier, len(met))

    gather_q = Gather(place, w_qkv, wq, make_piece(*w_qkv.shape, True), q_send, q_recv)
    gather_o = Gather(place, w_out, wo, make_piece(*w_out.shape, False), o_send, o_recv)
    gather_q.first_hop()
    gather_q.share_own()
    gather_o.share_own()
    own_copies = []
    for index, (source, full) in enumerate(((w_qkv, wq), (w_out, wo))):
        rows = source.shape[0]
        mine = full.at[pl.ds(pl.multiple_of(seq * rows, 16), rows), :]
        own_copies.append(pltpu.make_async_copy(source, mine, local_sem.at[index]))
        own_copies[-1].start()

    def small(source, target, slot, device):
        return pltpu.make_async_remote_copy(
            src_ref=source, dst_ref=target, send_sem=s_send.at[slot], recv_sem=s_recv.at[slot],
            device_id=device, device_id_type=pl.DeviceIdType.MESH,
        )

    ids_on = small(ids_row, id2, 0, after)
    ids_on.start()

    tokens, width = hid.shape
    strip = 16

    @pl.loop(0, tokens // strip)
    def _(index):
        rows = pl.ds(pl.multiple_of(index * strip, strip), strip)
        nrm[rows, :] = rms_scale(hid[rows, :].astype(jnp.float32), pre[...]).astype(jnp.bfloat16)

    ids_on.wait()

    def pass_on(own, far, near, slot):
        @pl.when(core == 0)
        def _():
            small(own, near, slot, place["sibling"]).start()

        @pl.when(core == 1)
        def _():
            small(far, near, slot, place["sibling"]).start()

    pass_on(ids_row, id2, id1, 1)

    for hop in range(1, chips):
        gather_q.step(hop)
        if hop == chips - 1:
            gather_o.first_hop()
    gather_q.finish()
    for moving in own_copies:
        moving.wait()

    def project(column):
        return jnp.dot(
            nrm[...], wq[:, column : column + HEAD], preferred_element_type=jnp.float32
        )

    def turned(values):
        a, b = values[:, : HEAD // 2], values[:, HEAD // 2 :]
        c, s = cos[...], sin[...]
        return jnp.concatenate([a * c - b * s, b * c + a * s], axis=1).astype(jnp.bfloat16)

    keys_at = Q_HEADS * HEAD
    for head in range(KV_HEADS):
        columns = slice(head * HEAD, (head + 1) * HEAD)
        kv[:, columns] = turned(project(keys_at + head * HEAD))
    for head in range(KV_HEADS, 2 * KV_HEADS):
        columns = slice(head * HEAD, (head + 1) * HEAD)
        kv[:, columns] = project(keys_at + head * HEAD).astype(jnp.bfloat16)
    kv_on = small(kv, kv2, 2, after)
    kv_on.start()
    gather_o.step(1)
    for head in range(Q_HEADS):
        columns = slice(head * HEAD, (head + 1) * HEAD)
        qry[:, columns] = turned(project(head * HEAD))
        if head == 1:
            gather_o.step(2)
    gather_o.step(3)

    def block(head, source, allowed, first):
        group = head // (Q_HEADS // KV_HEADS)
        columns = slice(head * HEAD, (head + 1) * HEAD)
        keys = source[:, group * HEAD : (group + 1) * HEAD]
        values = source[:, (KV_HEADS + group) * HEAD : (KV_HEADS + group + 1) * HEAD]
        scores = lax.dot_general(
            qry[:, columns], keys, (((1,), (1,)), ((), ())), preferred_element_type=jnp.float32
        )
        capped = CAP * jnp.tanh(scores * (1.0 / (math.sqrt(HEAD) * CAP)))
        weights = jnp.where(allowed, jnp.exp(capped), 0.0)
        total = jnp.sum(weights, axis=1, keepdims=True)
        mixed = jnp.dot(weights.astype(jnp.bfloat16), values, preferred_element_type=jnp.float32)
        if first:
            acc[:, columns] = mixed
            tot[:, head * 128 : (head + 1) * 128] = jnp.broadcast_to(total, (tokens, 128))
        else:
            acc[:, columns] += mixed
            tot[:, head * 128 : (head + 1) * 128] += jnp.broadcast_to(total, (tokens, 128))

    query_ids = ids_col[:, :1]
    row = lax.broadcasted_iota(jnp.int32, (tokens, tokens), 0)
    column = lax.broadcasted_iota(jnp.int32, (tokens, tokens), 1)
    own_allowed = (column <= row) & (query_ids == ids_row[:1, :])
    for head in range(Q_HEADS):
        block(head, kv, own_allowed, True)
        if head == 1:
            gather_o.step(4)
    gather_o.step(5)
    small(ids_row, id1, 1, place["sibling"]).wait()
    kv_on.wait()
    pass_on(kv, kv2, kv1, 3)
    far_allowed = (query_ids == id2[:1, :]) & (row + seq >= row + 2)
    for head in range(Q_HEADS):
        block(head, kv2, far_allowed, False)
    gather_o.step(6)
    small(kv, kv1, 3, place["sibling"]).wait()
    near_allowed = (query_ids == id1[:1, :]) & (row + seq >= row + 1)
    for head in range(Q_HEADS):
        block(head, kv1, near_allowed, False)
        columns = slice(head * HEAD, (head + 1) * HEAD)
        att[:, columns] = (acc[:, columns] / tot[:, head * 128 : head * 128 + 1]).astype(
            jnp.bfloat16
        )
    gather_o.step(7)
    gather_o.finish()
    for start in range(0, width, 256):
        branch[:, start : start + 256] = jnp.dot(
            att[...], wo[:, start : start + 256], preferred_element_type=jnp.float32
        )

    @pl.loop(0, tokens // strip)
    def _(index):
        rows = pl.ds(pl.multiple_of(index * strip, strip), strip)
        scaled = rms_scale(branch[rows, :], post[...])
        out[rows, :] = (hid[rows, :].astype(jnp.float32) + scaled).astype(jnp.bfloat16)

    gather_q.drain()
    gather_o.drain()


def ring_layer(hidden_in, segment_ids, pre_gain, w_qkv, w_out, post_gain):
    tokens, width = hidden_in.shape[1:]
    seq_count = lax.axis_size("seq")
    chips = seq_count // 2
    positions = lax.axis_index("seq") * tokens + jnp.arange(tokens, dtype=jnp.int32)
    inverse = 1.0 / 10000.0 ** (jnp.arange(HEAD // 2, dtype=jnp.float32) * 2.0 / HEAD)
    angles = positions.astype(jnp.float32)[:, None] * inverse[None, :]
    ids = segment_ids[0]
    pieces = 12 * (chips - 1) + 1
    bf16, f32 = jnp.bfloat16, jnp.float32
    vmem, dma = pltpu.VMEM, pltpu.SemaphoreType.DMA
    heads = Q_HEADS * HEAD
    pairs = 2 * KV_HEADS * HEAD
    result = pl.pallas_call(
        functools.partial(layer_kernel, chips),
        out_shape=jax.ShapeDtypeStruct((tokens, width), bf16),
        in_specs=[pl.BlockSpec(memory_space=vmem)] * 9,
        out_specs=pl.BlockSpec(memory_space=vmem),
        scratch_shapes=[
            vmem((width, w_qkv.shape[1]), bf16),
            vmem((heads, width), bf16),
            vmem((tokens, width), bf16),
            vmem((tokens, heads), bf16),
            vmem((tokens, pairs), bf16),
            vmem((tokens, pairs), bf16),
            vmem((tokens, pairs), bf16),
            vmem((8, tokens), jnp.int32),
            vmem((8, tokens), jnp.int32),
            vmem((tokens, heads), f32),
            vmem((tokens, Q_HEADS * 128), f32),
            vmem((tokens, heads), bf16),
            vmem((tokens, width), f32),
            dma((pieces,)),
            dma((pieces,)),
            dma((pieces,)),
            dma((pieces,)),
            dma((4,)),
            dma((4,)),
            dma((2,)),
        ],
        compiler_params=pltpu.CompilerParams(
            collective_id=0, has_side_effects=True, vmem_limit_bytes=58 * 1024 * 1024
        ),
    )(
        hidden_in[0],
        jnp.broadcast_to(ids[None, :], (8, tokens)),
        jnp.broadcast_to(ids[:, None], (tokens, 128)),
        jnp.cos(angles),
        jnp.sin(angles),
        pre_gain[None, :],
        w_qkv,
        w_out,
        post_gain[None, :],
    )
    return result[None]


def per_device(hidden_in, segment_ids, pre_gain, w_qkv, w_out, post_gain):
    tokens = hidden_in.shape[1]
    seq_count = lax.axis_size("seq")
    doc_most = min(WINDOW, seq_count * tokens // 8)
    whole_tiles = w_qkv.shape[0] % 48 == 0 and w_out.shape[0] % 16 == 0
    two_hops = doc_most - 1 <= 2 * tokens and 3 * tokens <= WINDOW
    if whole_tiles and two_hops and seq_count % 4 == 0 and lax.axis_size("batch") == 2:
        layer = ring_layer
    else:
        layer = plain_layer
    return layer(hidden_in, segment_ids, pre_gain, w_qkv, w_out, post_gain)


def solution(mesh):
    placed = (P("batch", "seq", None), P("batch", "seq"), P(), P("seq", None), P("seq", None), P())
    return jax.shard_map(
        per_device, mesh=mesh, in_specs=placed, out_specs=P("batch", "seq", None), check_vma=False
    )
```

```python
import functools
import math

import jax
import jax.numpy as jnp
from jax import lax
from jax.experimental import pallas as pl
from jax.experimental.pallas import tpu as pltpu
from jax.sharding import PartitionSpec as P

Q_HEADS = 4
KV_HEADS = 2
HEAD = 256
WINDOW = 4096
DOCS = 16


EPS = 1e-06
CAP = 50.0


def from_behind(block, axis, distance):
    devices = range(lax.axis_size(axis))
    route = [(i - distance, i) for i in devices if i - distance in devices]
    return lax.ppermute(block, axis, route)


def rms_scale(values, gain):
    return values * lax.rsqrt(jnp.mean(values * values, axis=-1, keepdims=True) + EPS) * gain


def rotary(values, positions, leading):
    head_size = values.shape[-1]
    half_dim = head_size // 2
    inverse = 1.0 / 10000.0 ** (jnp.arange(half_dim, dtype=jnp.float32) * 2.0 / head_size)
    angles = positions.astype(jnp.float32)[:, None] * inverse[None, :]
    shape = (
        (1,) * leading + (positions.shape[0],) + (1,) * (values.ndim - 2 - leading) + (half_dim,)
    )
    cosine = jnp.cos(angles).reshape(shape)
    sine = jnp.sin(angles).reshape(shape)
    first_half = values[..., :half_dim]
    second_half = values[..., half_dim:]
    return jnp.concatenate(
        [first_half * cosine - second_half * sine, second_half * cosine + first_half * sine],
        axis=-1,
    )


def plain_layer(hidden_in, segment_ids, pre_gain, w_qkv, w_out, post_gain):
    tok_rows = hidden_in.shape[1]
    seq_count = lax.axis_size("seq")
    seq_index = lax.axis_index("seq")
    groups = Q_HEADS // KV_HEADS
    doc_most = min(WINDOW, seq_count * tok_rows // 8)
    hops = min(-(-(doc_most - 1) // tok_rows), seq_count - 1)
    positions = seq_index * tok_rows + jnp.arange(tok_rows, dtype=jnp.int32)
    own_ids = segment_ids[0]
    id_blocks = [from_behind(own_ids, "seq", d) for d in range(hops, 0, -1)] + [own_ids]
    widened = hidden_in[0].astype(jnp.float32)
    normed = rms_scale(widened, pre_gain).astype(jnp.bfloat16)
    projected = jnp.dot(
        normed,
        lax.all_gather(w_qkv, "seq", axis=0, tiled=True),
        preferred_element_type=jnp.float32,
    )
    queries = rotary(
        projected[:, : Q_HEADS * HEAD].reshape(tok_rows, KV_HEADS, groups, HEAD), positions, 0
    ).astype(jnp.bfloat16)
    key_rows = rotary(
        projected[:, Q_HEADS * HEAD : (Q_HEADS + KV_HEADS) * HEAD].reshape(
            tok_rows, KV_HEADS, HEAD
        ),
        positions,
        0,
    ).astype(jnp.bfloat16)
    value_rows = projected[:, (Q_HEADS + KV_HEADS) * HEAD :].astype(jnp.bfloat16)
    both = jnp.concatenate([key_rows.reshape(tok_rows, KV_HEADS * HEAD), value_rows], axis=1)
    blocks = [from_behind(both, "seq", d) for d in range(hops, 0, -1)] + [both]
    kv = jnp.concatenate(blocks, axis=0).reshape(-1, 2, KV_HEADS, HEAD)
    ids = jnp.concatenate(id_blocks, axis=0)
    key_pos = (seq_index - hops) * tok_rows + jnp.arange((hops + 1) * tok_rows, dtype=jnp.int32)
    allowed = (
        (key_pos[None, :] >= 0)
        & (key_pos[None, :] <= positions[:, None])
        & (positions[:, None] - key_pos[None, :] < WINDOW)
        & (ids[None, :] == own_ids[:, None])
    )
    scores = jnp.einsum(
        "qhgd,khd->hgqk", queries, kv[:, 0], preferred_element_type=jnp.float32
    ) * (1.0 / math.sqrt(HEAD))
    capped = CAP * jnp.tanh(scores / CAP)
    weights = jnp.where(allowed[None, None], jnp.exp(capped), 0.0)
    totals = jnp.sum(weights, axis=-1)
    mixed = jnp.einsum(
        "hgqk,khd->hgqd", weights.astype(jnp.bfloat16), kv[:, 1], preferred_element_type=jnp.float32
    )
    attended = (mixed / totals[..., None]).astype(jnp.bfloat16)
    attended = attended.transpose(2, 0, 1, 3).reshape(tok_rows, Q_HEADS * HEAD)
    branch = jnp.dot(
        attended,
        lax.all_gather(w_out, "seq", axis=0, tiled=True),
        preferred_element_type=jnp.float32,
    )
    return (widened + rms_scale(branch, post_gain)).astype(jnp.bfloat16)[None]


class Gather:
    def __init__(self, place, own_ref, full_ref, piece, send_sems, recv_sems):
        self.place, self.own_ref, self.full_ref = place, own_ref, full_ref
        self.piece, self.send_sems, self.recv_sems = piece, send_sems, recv_sems
        self.steps = place["chips"] - 1
        self.started = []

    def slot(self, kind, hop, unit):
        return (kind * self.steps + hop - 1) * 2 + unit

    def spot(self, kind, hop, core, unit):
        place = self.place
        shift = -hop if kind == 0 else hop
        third = (1, 2 * place["x"], 2 - 2 * place["x"])[kind]
        device = place["chip_at"](place["ring"] + shift) * 2 + core
        return self.piece(self.full_ref, device, third, unit)

    def copy(self, source, target, slot, device):
        return pltpu.make_async_remote_copy(
            src_ref=source,
            dst_ref=target,
            send_sem=self.send_sems.at[slot],
            recv_sem=self.recv_sems.at[slot],
            device_id=device,
            device_id_type=pl.DeviceIdType.MESH,
        )

    def send(self, source, target, slot, device):
        moving = self.copy(source, target, slot, device)
        moving.start()
        self.started.append(moving)

    def arrived(self, spot, slot):
        self.copy(spot, spot, slot, self.place["sibling"]).wait_recv()

    def first_hop(self):
        place = self.place
        for unit in (1, 0):
            if unit == 0:
                for moving in self.started[-2:]:
                    moving.wait_send()
                del self.started[-2:]
            for kind, target in ((0, place["up"]), (1, place["down"])):
                third = (1, 2 * place["x"])[kind]
                self.send(
                    self.piece(self.own_ref, 0, third, unit),
                    self.piece(self.full_ref, place["seq"], third, unit),
                    self.slot(kind, 1, unit),
                    target,
                )

    def share_own(self):
        rows = self.own_ref.shape[0]
        mine = self.full_ref.at[pl.ds(pl.multiple_of(self.place["seq"] * rows, 16), rows), :]
        self.send(self.own_ref, mine, 12 * self.steps, self.place["sibling"])

    def relay(self, kind, hop, unit):
        spot = self.spot(kind, hop, self.place["core"], unit)
        self.send(spot, spot, self.slot(kind + 3, hop, unit), self.place["sibling"])

    def take_x(self, hop, units=(1, 0)):
        for unit in units:
            self.arrived(self.spot(2, hop, self.place["core"], unit), self.slot(2, hop, unit))
            self.relay(2, hop, unit)

    def step(self, hop):
        place = self.place
        for unit in (1, 0):
            if hop > 1:
                self.take_x(hop - 1, (unit,))
            for kind, target in ((0, place["up"]), (1, place["down"])):
                spot = self.spot(kind, hop, place["core"], unit)
                self.arrived(spot, self.slot(kind, hop, unit))
                if hop < self.steps:
                    self.send(spot, spot, self.slot(kind, hop + 1, unit), target)
                if kind == 1:
                    self.send(spot, spot, self.slot(2, hop, unit), place["across"])
                self.relay(kind, hop, unit)

    def finish(self, units=(1, 0)):
        self.take_x(self.steps, units)
        other = 1 - self.place["core"]
        for unit in units:
            for hop in range(1, self.steps + 1):
                for kind in range(3):
                    self.arrived(self.spot(kind, hop, other, unit), self.slot(kind + 3, hop, unit))
        if 1 not in units:
            return
        rows = self.own_ref.shape[0]
        start = (self.place["seq"] + 1 - 2 * self.place["core"]) * rows
        theirs = self.full_ref.at[pl.ds(pl.multiple_of(start, 16), rows), :]
        self.arrived(theirs, 12 * self.steps)

    def drain(self):
        for moving in self.started:
            moving.wait_send()


def make_piece(rows, width, by_rows):
    def piece(ref, device, third, unit):
        if by_rows:
            part, columns = rows // 3, width // 2
            return ref.at[
                pl.ds(pl.multiple_of(device * rows + third * part, 16), part),
                pl.ds(unit * columns, columns),
            ]
        columns = width // 6
        return ref.at[
            pl.ds(pl.multiple_of(device * rows, 16), rows),
            pl.ds(pl.multiple_of(third * 2 * columns + unit * columns, 128), columns),
        ]

    return piece


def layer_kernel(
    chips, hid, ids_row, ids_col, cos, sin, pre, w_qkv, w_out, post, out,
    wq, wo, nrm, qry, kv, kv1, kv2, id1, id2, acc, tot, att, branch,
    q_send, q_recv, o_send, o_recv, s_send, s_recv, local_sem,
):
    seq, x = lax.axis_index("seq"), lax.axis_index("batch")
    chip, core = seq // 2, seq % 2
    half = chips // 2
    layer, side = chip // 2, chip % 2
    ring = (1 - side) * layer + side * (chips - 1 - layer)

    def chip_at(position):
        position = (position + chips) % chips
        far = position // half
        return (1 - far) * 2 * position + far * (2 * (chips - 1 - position) + 1)

    def at(device_chip, device_core, batch):
        return {"seq": device_chip * 2 + device_core, "batch": batch}

    place = dict(
        chips=chips, seq=seq, x=x, core=core, ring=ring, chip_at=chip_at,
        sibling=at(chip, 1 - core, x), across=at(chip, core, 1 - x),
        up=at(chip_at(ring + 1), core, x), down=at(chip_at(ring - 1), core, x),
    )
    after = at((chip + 1) % chips, core, x)
    before = at((chip + chips - 1) % chips, core, x)
    met = [place["sibling"], place["across"], place["up"], place["down"], after, before]
    barrier = pltpu.get_barrier_semaphore()
    for other in met:
        pl.semaphore_signal(barrier, 1, device_id=other, device_id_type=pl.DeviceIdType.MESH)
    pl.semaphore_wait(barrier, len(met))

    gather_q = Gather(place, w_qkv, wq, make_piece(*w_qkv.shape, True), q_send, q_recv)
    gather_o = Gather(place, w_out, wo, make_piece(*w_out.shape, False), o_send, o_recv)
    gather_q.share_own()
    gather_o.share_own()
    gather_q.first_hop()
    own_copies = []
    for index, (source, full) in enumerate(((w_qkv, wq), (w_out, wo))):
        rows = source.shape[0]
        mine = full.at[pl.ds(pl.multiple_of(seq * rows, 16), rows), :]
        own_copies.append(pltpu.make_async_copy(source, mine, local_sem.at[index]))
        own_copies[-1].start()

    def small(source, target, slot, device):
        return pltpu.make_async_remote_copy(
            src_ref=source, dst_ref=target, send_sem=s_send.at[slot], recv_sem=s_recv.at[slot],
            device_id=device, device_id_type=pl.DeviceIdType.MESH,
        )

    ids_on = small(ids_row, id2, 0, after)
    ids_on.start()

    tokens, width = hid.shape
    strip = 16

    @pl.loop(0, tokens // strip)
    def _(index):
        rows = pl.ds(pl.multiple_of(index * strip, strip), strip)
        nrm[rows, :] = rms_scale(hid[rows, :].astype(jnp.float32), pre[...]).astype(jnp.bfloat16)

    ids_on.wait()

    def pass_on(own, far, near, slot):
        @pl.when(core == 0)
        def _():
            small(own, near, slot, place["sibling"]).start()

        @pl.when(core == 1)
        def _():
            small(far, near, slot, place["sibling"]).start()

    pass_on(ids_row, id2, id1, 1)

    for hop in range(1, chips):
        gather_q.step(hop)
        if hop == 1:
            gather_o.first_hop()
        elif hop > 1:
            gather_o.step(hop - 1)
    gather_q.finish((1,))
    for moving in own_copies:
        moving.wait()

    def project(column):
        return jnp.dot(
            nrm[...], wq[:, column : column + HEAD], preferred_element_type=jnp.float32
        )

    def turned(values):
        a, b = values[:, : HEAD // 2], values[:, HEAD // 2 :]
        c, s = cos[...], sin[...]
        return jnp.concatenate([a * c - b * s, b * c + a * s], axis=1).astype(jnp.bfloat16)

    keys_at = Q_HEADS * HEAD
    for head in range(KV_HEADS):
        columns = slice(head * HEAD, (head + 1) * HEAD)
        kv[:, columns] = turned(project(keys_at + head * HEAD))
    for head in range(KV_HEADS, 2 * KV_HEADS):
        columns = slice(head * HEAD, (head + 1) * HEAD)
        kv[:, columns] = project(keys_at + head * HEAD).astype(jnp.bfloat16)
    kv_on = small(kv, kv2, 2, after)
    kv_on.start()
    for hop in range(chips - 1, chips):
        gather_o.step(hop)
    gather_q.finish((0,))
    for head in range(Q_HEADS):
        columns = slice(head * HEAD, (head + 1) * HEAD)
        qry[:, columns] = turned(project(head * HEAD))

    def block(head, source, allowed, first):
        group = head // (Q_HEADS // KV_HEADS)
        columns = slice(head * HEAD, (head + 1) * HEAD)
        keys = source[:, group * HEAD : (group + 1) * HEAD]
        values = source[:, (KV_HEADS + group) * HEAD : (KV_HEADS + group + 1) * HEAD]
        scores = lax.dot_general(
            qry[:, columns], keys, (((1,), (1,)), ((), ())), preferred_element_type=jnp.float32
        )
        capped = CAP * jnp.tanh(scores * (1.0 / (math.sqrt(HEAD) * CAP)))
        weights = jnp.where(allowed, jnp.exp(capped), 0.0)
        total = jnp.sum(weights, axis=1, keepdims=True)
        mixed = jnp.dot(weights.astype(jnp.bfloat16), values, preferred_element_type=jnp.float32)
        if first:
            acc[:, columns] = mixed
            tot[:, head * 128 : (head + 1) * 128] = jnp.broadcast_to(total, (tokens, 128))
        else:
            acc[:, columns] += mixed
            tot[:, head * 128 : (head + 1) * 128] += jnp.broadcast_to(total, (tokens, 128))

    query_ids = ids_col[:, :1]
    row = lax.broadcasted_iota(jnp.int32, (tokens, tokens), 0)
    column = lax.broadcasted_iota(jnp.int32, (tokens, tokens), 1)
    own_allowed = (column <= row) & (query_ids == ids_row[:1, :])
    for head in range(Q_HEADS):
        block(head, kv, own_allowed, True)
    small(ids_row, id1, 1, place["sibling"]).wait()
    kv_on.wait()
    pass_on(kv, kv2, kv1, 3)
    far_allowed = (query_ids == id2[:1, :]) & (row + seq >= row + 2)
    for head in range(Q_HEADS):
        block(head, kv2, far_allowed, False)
    small(kv, kv1, 3, place["sibling"]).wait()
    near_allowed = (query_ids == id1[:1, :]) & (row + seq >= row + 1)
    for head in range(Q_HEADS):
        block(head, kv1, near_allowed, False)
        columns = slice(head * HEAD, (head + 1) * HEAD)
        att[:, columns] = (acc[:, columns] / tot[:, head * 128 : head * 128 + 1]).astype(
            jnp.bfloat16
        )
    gather_o.finish()
    for start in range(0, width, 256):
        branch[:, start : start + 256] = jnp.dot(
            att[...], wo[:, start : start + 256], preferred_element_type=jnp.float32
        )

    @pl.loop(0, tokens // strip)
    def _(index):
        rows = pl.ds(pl.multiple_of(index * strip, strip), strip)
        scaled = rms_scale(branch[rows, :], post[...])
        out[rows, :] = (hid[rows, :].astype(jnp.float32) + scaled).astype(jnp.bfloat16)

    gather_q.drain()
    gather_o.drain()


def ring_layer(hidden_in, segment_ids, pre_gain, w_qkv, w_out, post_gain):
    tokens, width = hidden_in.shape[1:]
    seq_count = lax.axis_size("seq")
    chips = seq_count // 2
    positions = lax.axis_index("seq") * tokens + jnp.arange(tokens, dtype=jnp.int32)
    inverse = 1.0 / 10000.0 ** (jnp.arange(HEAD // 2, dtype=jnp.float32) * 2.0 / HEAD)
    angles = positions.astype(jnp.float32)[:, None] * inverse[None, :]
    ids = segment_ids[0]
    pieces = 12 * (chips - 1) + 1
    bf16, f32 = jnp.bfloat16, jnp.float32
    vmem, dma = pltpu.VMEM, pltpu.SemaphoreType.DMA
    heads = Q_HEADS * HEAD
    pairs = 2 * KV_HEADS * HEAD
    result = pl.pallas_call(
        functools.partial(layer_kernel, chips),
        out_shape=jax.ShapeDtypeStruct((tokens, width), bf16),
        in_specs=[pl.BlockSpec(memory_space=vmem)] * 9,
        out_specs=pl.BlockSpec(memory_space=vmem),
        scratch_shapes=[
            vmem((width, w_qkv.shape[1]), bf16),
            vmem((heads, width), bf16),
            vmem((tokens, width), bf16),
            vmem((tokens, heads), bf16),
            vmem((tokens, pairs), bf16),
            vmem((tokens, pairs), bf16),
            vmem((tokens, pairs), bf16),
            vmem((1, tokens), jnp.int32),
            vmem((1, tokens), jnp.int32),
            vmem((tokens, heads), f32),
            vmem((tokens, Q_HEADS * 128), f32),
            vmem((tokens, heads), bf16),
            vmem((tokens, width), f32),
            dma((pieces,)),
            dma((pieces,)),
            dma((pieces,)),
            dma((pieces,)),
            dma((4,)),
            dma((4,)),
            dma((2,)),
        ],
        compiler_params=pltpu.CompilerParams(
            collective_id=0, has_side_effects=True, vmem_limit_bytes=58 * 1024 * 1024
        ),
    )(
        hidden_in[0],
        segment_ids,
        jnp.broadcast_to(ids[:, None], (tokens, 128)),
        jnp.cos(angles),
        jnp.sin(angles),
        pre_gain,
        w_qkv,
        w_out,
        post_gain,
    )
    return result[None]


def per_device(hidden_in, segment_ids, pre_gain, w_qkv, w_out, post_gain):
    tokens = hidden_in.shape[1]
    seq_count = lax.axis_size("seq")
    doc_most = min(WINDOW, seq_count * tokens // 8)
    whole_tiles = w_qkv.shape[0] % 48 == 0 and w_out.shape[0] % 16 == 0
    two_hops = doc_most - 1 <= 2 * tokens and 3 * tokens <= WINDOW
    if whole_tiles and two_hops and seq_count % 4 == 0 and seq_count > 12 and lax.axis_size("batch") == 2:
        layer = ring_layer
    else:
        layer = plain_layer
    return layer(hidden_in, segment_ids, pre_gain, w_qkv, w_out, post_gain)


def solution(mesh):
    placed = (P("batch", "seq", None), P("batch", "seq"), P(), P("seq", None), P("seq", None), P())
    return jax.shard_map(
        per_device, mesh=mesh, in_specs=placed, out_specs=P("batch", "seq", None), check_vma=False
    )
```
